32 devices in a mesh: sx: 8 (over z, y), sy: 4 (over x, core).
Axes of the slice: x: 2, y: 2, z: 4, core: 2. Of those that a mesh axis runs over, the one named last changes fastest.
Arguments:
- tensors: bfloat16 [2, 8, 4, 1024, 256], P(None, 'sx', 'sy'), may hold values from -6 to 6
- gates: bfloat16 [5, 2, 2, 256, 256], replicated, may hold values from -0.1875 to 0.1875
- closing_rows: bfloat16 [2, 4096, 1024], P(None, ('sx', 'sy')), may hold values from -0.125 to 0.125
- closing_columns: float32 [2, 4096, 256], P(None, ('sx', 'sy')), may hold values from -0.25 to 0.25
Outputs:
- amplitudes: float32 [2, 4096], replicated
The draws below stay inside these ranges and needn't reach their ends.
All inputs are finite; a program needn't handle non-finite values.
Results may differ from the reference program's by a relative error of at most 0.012.
Values may be sent and summed in bfloat16 or wider, within the bound.
A program may use at most 64 MiB of HBM per device.

```python
import jax
import jax.numpy as jnp
from jax import lax

C = 256
R = 1024
AMPS = 4096
BX = 3
SECTIONS = 5
AMP_DEV = 128
N_SX = 8
N_SY = 4


def shard_levels(stream_key, dims, pieces, smallest, largest):
    factor_of = 1.0
    for position, parts in pieces:
        heights = jax.random.uniform(jax.random.fold_in(jax.random.fold_in(stream_key, 6), position), (parts,), jnp.float32, smallest / len(pieces), largest / len(pieces))
        factor_of = factor_of * jnp.repeat(jnp.exp(heights), dims[position] // parts).reshape((-1,) + (1,) * (len(dims) - 1 - position))
    return factor_of


def scatter_about(stream_key, shape, deviation, limit, cuts=(), dtype=jnp.bfloat16):
    level = shard_levels(stream_key, shape, cuts, -0.22, 0.18) if cuts else 1.0
    entries = jax.random.normal(stream_key, shape, jnp.float32) * deviation * level
    return jnp.minimum(jnp.maximum(entries, -limit), limit).astype(dtype)


def setup_inputs(seed: int = 0) -> dict:
    key_of = jax.random.split(jax.random.key(seed), 5)
    return {
        "tensors": scatter_about(key_of[0], (2, N_SX, N_SY, R, C), 1.0, 6.0, ((1, 8), (2, 4))),
        "gates": scatter_about(key_of[1], (SECTIONS, 2, 2, C, C), (4 * C) ** -0.5, 0.1875),
        "closing_rows": scatter_about(key_of[2], (2, AMPS, R), (2 * R) ** -0.5, 0.125, ((1, 32),)),
        "closing_columns": scatter_about(key_of[3], (2, AMPS, C), (2 * C) ** -0.5, 0.25, ((1, 32),), jnp.float32),
    }


HIGH = lax.Precision.HIGHEST


def complex_product(values, matrix):
    values = values.astype(jnp.float32)
    matrix = matrix.astype(jnp.float32)
    real_part = jnp.matmul(values[0], matrix[0], precision=HIGH) - jnp.matmul(values[1], matrix[1], precision=HIGH)
    imag_part = jnp.matmul(values[0], matrix[1], precision=HIGH) + jnp.matmul(values[1], matrix[0], precision=HIGH)
    return jnp.stack([real_part, imag_part])


def apply_section(current, gate_pair, axis_dim, bit_pos):
    shape = current.shape
    count = shape[axis_dim]
    split = shape[:axis_dim] + (count >> (bit_pos + 1), 2, 1 << bit_pos) + shape[axis_dim + 1:]
    blocks = current.reshape(split)
    lower = jnp.take(blocks, 0, axis=axis_dim + 1)
    upper = jnp.take(blocks, 1, axis=axis_dim + 1)
    new_lower = complex_product(lower, gate_pair[0]) + complex_product(upper, gate_pair[1])
    new_upper = complex_product(upper, gate_pair[0]) - complex_product(lower, gate_pair[1])
    joined = jnp.stack([new_lower, new_upper], axis=axis_dim + 1).reshape(shape)
    return joined.astype(jnp.bfloat16)


def reference(tensors, gates, closing_rows, closing_columns):
    current = tensors
    for number in range(SECTIONS):
        if number < BX:
            current = apply_section(current, gates[number], 1, number)
        else:
            current = apply_section(current, gates[number], 2, number - BX)
    slices = N_SX * N_SY
    flat = current.reshape(2, slices, R, C).astype(jnp.float32)
    row_close = closing_rows.reshape(2, slices, AMP_DEV, R).astype(jnp.float32)
    column_close = closing_columns.reshape(2, slices, AMP_DEV, C)
    proj_real = jnp.matmul(row_close[0], flat[0], precision=HIGH) - jnp.matmul(row_close[1], flat[1], precision=HIGH)
    proj_imag = jnp.matmul(row_close[0], flat[1], precision=HIGH) + jnp.matmul(row_close[1], flat[0], precision=HIGH)
    amp_real = jnp.sum(proj_real * column_close[0] - proj_imag * column_close[1], axis=-1)
    amp_imag = jnp.sum(proj_real * column_close[1] + proj_imag * column_close[0], axis=-1)
    return jnp.stack([amp_real, amp_imag]).reshape(2, AMPS)
```

```python
import functools

import jax
import jax.numpy as jnp
from jax import lax
from jax.experimental import pallas as pl
from jax.experimental.pallas import tpu as pltpu
from jax.sharding import PartitionSpec as P

MESH = pl.DeviceIdType.MESH
CHUNKS = 8
LAG = 2


def kernel(
    plan,
    x_hbm,
    g_hbm,
    u_hbm,
    v_hbm,
    out_ref,
    xs,
    xr,
    gates,
    mix,
    back,
    ubuf,
    vraw,
    vbuf,
    wbuf,
    part,
    red,
    local_sem,
    xsend,
    xrecv,
    gsend,
    grecv,
    psend,
    precv,
):
    exchanges, gathers = plan
    rows, width2 = xs.shape[1:]
    width = width2 // 2
    slots, _, amps, _ = ubuf.shape
    step_rows = rows // CHUNKS
    coords = {"sx": lax.axis_index("sx"), "sy": lax.axis_index("sy")}

    def bit_of(axis, pos):
        return (coords[axis] // (1 << pos)) % 2

    def far(*flips):
        where = dict(coords)
        for axis, pos in flips:
            where[axis] = where[axis] + (1 << pos) * (1 - 2 * bit_of(axis, pos))
        return (where["sx"], where["sy"])

    copies = [
        pltpu.make_async_copy(x_hbm.at[0], xs.at[0, :, pl.ds(0, width)], local_sem.at[0]),
        pltpu.make_async_copy(x_hbm.at[1], xs.at[0, :, pl.ds(width, width)], local_sem.at[1]),
        pltpu.make_async_copy(v_hbm, vraw, local_sem.at[2]),
        pltpu.make_async_copy(u_hbm, ubuf.at[0], local_sem.at[3]),
        pltpu.make_async_copy(g_hbm, gates, local_sem.at[4]),
    ]
    for copy in copies:
        copy.start()

    barrier = pltpu.get_barrier_semaphore()
    peers = [(axis, pos) for axis, pos, _ in exchanges + gathers]
    for peer in peers:
        pl.semaphore_signal(barrier, inc=1, device_id=far(peer), device_id_type=MESH)
    copies[2].wait()
    vbuf[0] = vraw[...].astype(jnp.bfloat16)
    copies[0].wait()
    copies[1].wait()
    copies[3].wait()
    pl.semaphore_wait(barrier, len(peers))

    def x_copy(stage, chunk):
        here = pl.ds(chunk * step_rows, step_rows)
        return pltpu.make_async_remote_copy(
            src_ref=xs.at[stage, here],
            dst_ref=xr.at[stage, here],
            send_sem=xsend.at[stage, chunk],
            recv_sem=xrecv.at[stage, chunk],
            device_id=far(exchanges[stage][:2]),
            device_id_type=MESH,
        )

    def g_copy(step, slot, piece):
        landing = slot + (1 << step)
        if piece == 0:
            src, dst = vbuf.at[slot], vbuf.at[landing]
        else:
            src, dst = ubuf.at[slot, piece - 1], ubuf.at[landing, piece - 1]
        return pltpu.make_async_remote_copy(
            src_ref=src,
            dst_ref=dst,
            send_sem=gsend.at[landing, piece],
            recv_sem=grecv.at[landing, piece],
            device_id=far(gathers[step][:2]),
            device_id_type=MESH,
        )

    for chunk in range(CHUNKS):
        x_copy(0, chunk).start()
    for piece in range(3):
        for step in range(len(gathers)):
            g_copy(step, 0, piece).start()

    def arrive(slot, piece):
        step = slot.bit_length() - 1
        g_copy(step, slot - (1 << step), piece).wait_recv()
        for later in range(step + 1, len(gathers)):
            g_copy(later, slot, piece).start()

    copies[4].wait()
    for stage, (axis, pos, number) in enumerate(exchanges):
        sign = (1 - 2 * bit_of(axis, pos)).astype(jnp.float32).astype(jnp.bfloat16)
        for half in range(2):
            real, imag = gates[number, half, 0], gates[number, half, 1]
            if half:
                real, imag = real * sign, imag * sign
            base = half * width2
            mix[stage, pl.ds(base, width), pl.ds(0, width)] = real
            mix[stage, pl.ds(base, width), pl.ds(width, width)] = imag
            mix[stage, pl.ds(base + width, width), pl.ds(0, width)] = -imag
            mix[stage, pl.ds(base + width, width), pl.ds(width, width)] = real
    for step, (axis, pos, number) in enumerate(gathers):
        sign = (2 * bit_of(axis, pos) - 1).astype(jnp.float32).astype(jnp.bfloat16)
        for half in range(2):
            real, imag = gates[number, half, 0], gates[number, half, 1]
            if half:
                real, imag = real * sign, imag * sign
            back[step, half, pl.ds(0, width), pl.ds(0, width)] = real
            back[step, half, pl.ds(0, width), pl.ds(width, width)] = -imag
            back[step, half, pl.ds(width, width), pl.ds(0, width)] = imag
            back[step, half, pl.ds(width, width), pl.ds(width, width)] = real

    order = sorted(range(len(gathers)), key=lambda step: -gathers[step][2])

    def pull_back(slot):
        values = jnp.concatenate([vbuf[slot, 0], vbuf[slot, 1]], axis=-1)
        for place, step in enumerate(order):
            half = (slot >> step) & 1
            product = lax.dot_general(
                values,
                back[step, half],
                (((1,), (1,)), ((), ())),
                preferred_element_type=jnp.float32,
            )
            values = product.astype(jnp.bfloat16)
        wbuf[slot] = product

    def section(stage, chunk):
        x_copy(stage, chunk).wait_recv()
        here = pl.ds(chunk * step_rows, step_rows)
        joined = jnp.concatenate([xs[stage, here], xr[stage, here]], axis=-1)
        xs[stage + 1, here] = jnp.dot(
            joined, mix[stage], preferred_element_type=jnp.float32
        ).astype(jnp.bfloat16)
        if stage + 1 < len(exchanges):
            x_copy(stage + 1, chunk).start()

    todo = [(slot, piece) for piece in range(3) for slot in range(1, slots)]
    forwards = [event for event in todo if event[0] < slots // 2]
    ends = [event for event in todo if event[0] >= slots // 2]
    total = CHUNKS + LAG * (len(exchanges) - 1)
    done = 0
    pull_back(0)
    for tick in range(total):
        for stage in range(len(exchanges)):
            chunk = tick - LAG * stage
            if 0 <= chunk < CHUNKS:
                section(stage, chunk)
        until = len(forwards) * (tick + 1) // total
        for event in forwards[done:until]:
            arrive(*event)
        done = until
    for event in ends:
        if event[1] == 0:
            arrive(*event)
    for slot in range(1, slots):
        pull_back(slot)
    for event in ends:
        if event[1] > 0:
            arrive(*event)

    final = xs.at[len(exchanges)]

    def p_copy(slot):
        flips = [gathers[step][:2] for step in range(len(gathers)) if (slot >> step) & 1]
        return pltpu.make_async_remote_copy(
            src_ref=part.at[slot],
            dst_ref=red.at[slot],
            send_sem=psend.at[slot],
            recv_sem=precv.at[slot],
            device_id=far(*flips),
            device_id_type=MESH,
        )

    def fold(values):
        lanes = 128
        total_ = values[:, :lanes]
        for start in range(lanes, width, lanes):
            total_ = total_ + values[:, start : start + lanes]
        return jnp.sum(total_.T, axis=0, keepdims=True)

    for slot in reversed(range(slots)):
        by_real = jnp.dot(ubuf[slot, 0], final[...], preferred_element_type=jnp.float32)
        by_imag = jnp.dot(ubuf[slot, 1], final[...], preferred_element_type=jnp.float32)
        proj_real = by_real[:, :width] - by_imag[:, width:]
        proj_imag = by_real[:, width:] + by_imag[:, :width]
        w_real, w_imag = wbuf[slot, :, :width], wbuf[slot, :, width:]
        part[slot, 0:1] = fold(proj_real * w_real - proj_imag * w_imag)
        part[slot, 1:2] = fold(proj_real * w_imag + proj_imag * w_real)
        if slot:
            p_copy(slot).start()

    result = part[0]
    for slot in range(1, slots):
        p_copy(slot).wait_recv()
    for slot in range(1, slots):
        result = result + red[slot]
    out_ref[...] = result

    for stage in range(len(exchanges)):
        for chunk in range(CHUNKS):
            x_copy(stage, chunk).wait_send()
    for step in range(len(gathers)):
        for slot in range(1 << step):
            for piece in range(3):
                g_copy(step, slot, piece).wait_send()
    for slot in range(1, slots):
        p_copy(slot).wait_send()


def local(tensors, gates, closing_rows, closing_columns):
    current = tensors[:, 0, 0]
    rows, width = current.shape[1:]
    amps = closing_rows.shape[1]
    bits_x = lax.axis_size("sx").bit_length() - 1
    bits_y = lax.axis_size("sy").bit_length() - 1
    exchanges = [("sx", pos, pos) for pos in range(bits_x - 1)]
    gathers = [("sx", bits_x - 1, bits_x - 1)]
    gathers += [("sy", pos, bits_x + pos) for pos in reversed(range(bits_y))]
    stages, steps = len(exchanges), len(gathers)
    slots = 1 << steps
    closed = pl.pallas_call(
        functools.partial(kernel, (exchanges, gathers)),
        out_shape=jax.ShapeDtypeStruct((2, amps), jnp.float32),
        in_specs=[pl.BlockSpec(memory_space=pl.ANY)] * 4,
        out_specs=pl.BlockSpec(memory_space=pltpu.VMEM),
        scratch_shapes=[
            pltpu.VMEM((stages + 1, rows, 2 * width), jnp.bfloat16),
            pltpu.VMEM((stages, rows, 2 * width), jnp.bfloat16),
            pltpu.VMEM(gates.shape, jnp.bfloat16),
            pltpu.VMEM((stages, 4 * width, 2 * width), jnp.bfloat16),
            pltpu.VMEM((steps, 2, 2 * width, 2 * width), jnp.bfloat16),
            pltpu.VMEM((slots, 2, amps, rows), jnp.bfloat16),
            pltpu.VMEM((2, amps, width), jnp.float32),
            pltpu.VMEM((slots, 2, amps, width), jnp.bfloat16),
            pltpu.VMEM((slots, amps, 2 * width), jnp.float32),
            pltpu.VMEM((slots, 2, amps), jnp.float32),
            pltpu.VMEM((slots, 2, amps), jnp.float32),
            pltpu.SemaphoreType.DMA((5,)),
            pltpu.SemaphoreType.DMA((stages, CHUNKS)),
            pltpu.SemaphoreType.DMA((stages, CHUNKS)),
            pltpu.SemaphoreType.DMA((slots, 3)),
            pltpu.SemaphoreType.DMA((slots, 3)),
            pltpu.SemaphoreType.DMA((slots,)),
            pltpu.SemaphoreType.DMA((slots,)),
        ],
        compiler_params=pltpu.CompilerParams(
            collective_id=0, has_side_effects=True, vmem_limit_bytes=60 * 2**20
        ),
    )(current, gates, closing_rows, closing_columns)
    return lax.all_gather(closed, ("sx", "sy"), axis=1, tiled=True)


def solution(mesh):
    placed = (
        P(None, "sx", "sy", None, None),
        P(),
        P(None, ("sx", "sy"), None),
        P(None, ("sx", "sy"), None),
    )
    return jax.shard_map(local, mesh=mesh, in_specs=placed, out_specs=P(), check_vma=False)
```

```python
import functools

import jax
import jax.numpy as jnp
from jax import lax
from jax.experimental import pallas as pl
from jax.experimental.pallas import tpu as pltpu
from jax.sharding import PartitionSpec as P

MESH = pl.DeviceIdType.MESH
CHUNKS = 8
LAG = 5
HOLD = 4
FIRST = 6


def kernel(
    plan,
    x_hbm,
    g_hbm,
    u_hbm,
    v_hbm,
    out_ref,
    xs,
    xr,
    gates,
    mix,
    back,
    ubuf,
    vraw,
    vbuf,
    wbuf,
    acc,
    part,
    red,
    every,
    local_sem,
    xsend,
    xrecv,
    gsend,
    grecv,
    psend,
    precv,
    bsend,
    brecv,
):
    exchanges, gathers = plan
    rows, width2 = xs.shape[1:]
    width = width2 // 2
    slots, _, amps, _ = ubuf.shape
    step_rows = rows // CHUNKS
    coords = {"sx": lax.axis_index("sx"), "sy": lax.axis_index("sy")}

    def bit_of(axis, pos):
        return (coords[axis] // (1 << pos)) % 2

    def far(*flips):
        where = dict(coords)
        for axis, pos in flips:
            where[axis] = where[axis] + (1 << pos) * (1 - 2 * bit_of(axis, pos))
        return (where["sx"], where["sy"])

    copies = [
        pltpu.make_async_copy(x_hbm.at[0], xs.at[0, :, pl.ds(0, width)], local_sem.at[0]),
        pltpu.make_async_copy(x_hbm.at[1], xs.at[0, :, pl.ds(width, width)], local_sem.at[1]),
        pltpu.make_async_copy(v_hbm, vraw, local_sem.at[2]),
        pltpu.make_async_copy(u_hbm, ubuf.at[0], local_sem.at[3]),
        pltpu.make_async_copy(g_hbm, gates, local_sem.at[4]),
    ]
    for copy in copies:
        copy.start()

    barrier = pltpu.get_barrier_semaphore()
    peers = [(axis, pos) for axis, pos, _ in exchanges + gathers]
    for peer in peers:
        pl.semaphore_signal(barrier, inc=1, device_id=far(peer), device_id_type=MESH)
    copies[2].wait()
    vbuf[0] = vraw[...].astype(jnp.bfloat16)
    copies[0].wait()
    copies[1].wait()
    pl.semaphore_wait(barrier, len(peers))

    def x_copy(stage, chunk):
        here = pl.ds(chunk * step_rows, step_rows)
        return pltpu.make_async_remote_copy(
            src_ref=xs.at[stage, here],
            dst_ref=xr.at[stage, here],
            send_sem=xsend.at[stage, chunk],
            recv_sem=xrecv.at[stage, chunk],
            device_id=far(exchanges[stage][:2]),
            device_id_type=MESH,
        )

    def g_copy(step, slot, piece):
        landing = slot + (1 << step)
        if piece == 0:
            src, dst = vbuf.at[slot], vbuf.at[landing]
        else:
            src, dst = ubuf.at[slot, piece - 1], ubuf.at[landing, piece - 1]
        return pltpu.make_async_remote_copy(
            src_ref=src,
            dst_ref=dst,
            send_sem=gsend.at[landing, piece],
            recv_sem=grecv.at[landing, piece],
            device_id=far(gathers[step][:2]),
            device_id_type=MESH,
        )

    def offer(step):
        for piece in range(3):
            g_copy(step, 0, piece).start()

    for chunk in range(CHUNKS):
        x_copy(0, chunk).start()
    copies[3].wait()
    early = bit_of(*gathers[0][:2]) == bit_of(*exchanges[-1][:2])
    pl.when(early)(functools.partial(offer, 0))
    for step in range(1, len(gathers)):
        offer(step)

    def arrive(slot, piece):
        step = slot.bit_length() - 1
        g_copy(step, slot - (1 << step), piece).wait_recv()
        for later in range(step + 1, len(gathers)):
            g_copy(later, slot, piece).start()

    copies[4].wait()
    for stage, (axis, pos, number) in enumerate(exchanges):
        sign = (1 - 2 * bit_of(axis, pos)).astype(jnp.float32).astype(jnp.bfloat16)
        for half in range(2):
            real, imag = gates[number, half, 0], gates[number, half, 1]
            if half:
                real, imag = real * sign, imag * sign
            base = half * width2
            mix[stage, pl.ds(base, width), pl.ds(0, width)] = real
            mix[stage, pl.ds(base, width), pl.ds(width, width)] = imag
            mix[stage, pl.ds(base + width, width), pl.ds(0, width)] = -imag
            mix[stage, pl.ds(base + width, width), pl.ds(width, width)] = real
    for step, (axis, pos, number) in enumerate(gathers):
        sign = (2 * bit_of(axis, pos) - 1).astype(jnp.float32).astype(jnp.bfloat16)
        for half in range(2):
            real, imag = gates[number, half, 0], gates[number, half, 1]
            if half:
                real, imag = real * sign, imag * sign
            back[step, half, pl.ds(0, width), pl.ds(0, width)] = real
            back[step, half, pl.ds(0, width), pl.ds(width, width)] = -imag
            back[step, half, pl.ds(width, width), pl.ds(0, width)] = imag
            back[step, half, pl.ds(width, width), pl.ds(width, width)] = real

    order = sorted(range(len(gathers)), key=lambda step: -gathers[step][2])

    def pull_back(slot):
        values = jnp.concatenate([vbuf[slot, 0], vbuf[slot, 1]], axis=-1)
        for place, step in enumerate(order):
            half = (slot >> step) & 1
            product = lax.dot_general(
                values,
                back[step, half],
                (((1,), (1,)), ((), ())),
                preferred_element_type=jnp.float32,
            )
            values = product.astype(jnp.bfloat16)
        wbuf[slot] = product

    def section(stage, chunk):
        x_copy(stage, chunk).wait_recv()
        here = pl.ds(chunk * step_rows, step_rows)
        joined = jnp.concatenate([xs[stage, here], xr[stage, here]], axis=-1)
        xs[stage + 1, here] = jnp.dot(
            joined, mix[stage], preferred_element_type=jnp.float32
        ).astype(jnp.bfloat16)
        if stage + 1 < len(exchanges):
            x_copy(stage + 1, chunk).start()

    def spread(events, moments):
        size = len(moments)
        return {
            moment: events[len(events) * place // size : len(events) * (place + 1) // size]
            for place, moment in enumerate(moments)
        }

    total = CHUNKS + LAG * (len(exchanges) - 1)
    wait_tick = total - CHUNKS + FIRST - 1
    half = slots // 2
    relays = [(slot, piece) for piece in range(3) for slot in range(2, half) if slot % 2 == 0]
    late = [(slot, piece) for piece in range(3) for slot in range(1, half) if slot % 2]
    late.sort(key=lambda event: (event[1] + event[0].bit_count(), event[0]))
    ends = [(slot, piece) for piece in range(3) for slot in range(half, slots)]
    at_tick = spread(relays, range(HOLD + 1))
    at_tick.update(spread(late, range(HOLD + 1, wait_tick + 1)))
    pull_back(0)

    def gather_rows(slot, index, start, stop):
        return jnp.dot(
            ubuf[slot, index, :, start:stop],
            xs[len(exchanges), start:stop],
            preferred_element_type=jnp.float32,
        )

    for tick in range(total):
        for stage in range(len(exchanges)):
            chunk = tick - LAG * stage
            if 0 <= chunk < CHUNKS:
                section(stage, chunk)
        if tick == HOLD:
            pl.when(jnp.logical_not(early))(functools.partial(offer, 0))
        for event in at_tick.get(tick, ()):
            arrive(*event)
        if tick == wait_tick:
            for event in ends:
                arrive(*event)
            for slot in range(1, slots):
                pull_back(slot)
            for slot in range(slots):
                for index in range(2):
                    acc[slot, index] = gather_rows(slot, index, 0, FIRST * step_rows)

    def p_copy(slot):
        flips = [gathers[step][:2] for step in range(len(gathers)) if (slot >> step) & 1]
        return pltpu.make_async_remote_copy(
            src_ref=part.at[slot],
            dst_ref=red.at[slot],
            send_sem=psend.at[slot],
            recv_sem=precv.at[slot],
            device_id=far(*flips),
            device_id_type=MESH,
        )

    def fold(values):
        lanes = 128
        total_ = values[:, :lanes]
        for start in range(lanes, width, lanes):
            total_ = total_ + values[:, start : start + lanes]
        return jnp.sum(total_.T, axis=0, keepdims=True)

    for slot in reversed(range(slots)):
        by_real = acc[slot, 0] + gather_rows(slot, 0, FIRST * step_rows, rows)
        by_imag = acc[slot, 1] + gather_rows(slot, 1, FIRST * step_rows, rows)
        proj_real = by_real[:, :width] - by_imag[:, width:]
        proj_imag = by_real[:, width:] + by_imag[:, :width]
        w_real, w_imag = wbuf[slot, :, :width], wbuf[slot, :, width:]
        part[slot, 0:1] = fold(proj_real * w_real - proj_imag * w_imag)
        part[slot, 1:2] = fold(proj_real * w_imag + proj_imag * w_real)
        if slot:
            p_copy(slot).start()

    result = part[0]
    for slot in range(1, slots):
        p_copy(slot).wait_recv()
    for slot in range(1, slots):
        result = result + red[slot]
    count_y = lax.axis_size("sy")
    count = lax.axis_size("sx") * count_y
    rank = coords["sx"] * count_y + coords["sy"]
    every[pl.ds(rank, 1)] = result[None]

    def b_copy(offset):
        other = (rank + offset) % count
        return pltpu.make_async_remote_copy(
            src_ref=every.at[rank],
            dst_ref=every.at[rank],
            send_sem=bsend.at[offset],
            recv_sem=brecv.at[offset],
            device_id=(other // count_y, other % count_y),
            device_id_type=MESH,
        )

    @pl.loop(1, count)
    def _(offset):
        b_copy(offset).start()


    for stage in range(len(exchanges)):
        for chunk in range(CHUNKS):
            x_copy(stage, chunk).wait_send()
    for step in range(len(gathers)):
        for slot in range(1 << step):
            for piece in range(3):
                g_copy(step, slot, piece).wait_send()
    for slot in range(1, slots):
        p_copy(slot).wait_send()

    @pl.loop(1, count)
    def _(offset):
        b_copy(offset).wait()

    out_ref[0] = every[:, 0, :]
    out_ref[1] = every[:, 1, :]


def local(tensors, gates, closing_rows, closing_columns):
    current = tensors[:, 0, 0]
    rows, width = current.shape[1:]
    amps = closing_rows.shape[1]
    bits_x = lax.axis_size("sx").bit_length() - 1
    bits_y = lax.axis_size("sy").bit_length() - 1
    exchanges = [("sx", pos, pos) for pos in range(bits_x - 1)]
    gathers = [("sx", bits_x - 1, bits_x - 1)]
    gathers += [("sy", pos, bits_x + pos) for pos in reversed(range(bits_y))]
    stages, steps = len(exchanges), len(gathers)
    slots = 1 << steps
    count = lax.axis_size("sx") * lax.axis_size("sy")
    closed = pl.pallas_call(
        functools.partial(kernel, (exchanges, gathers)),
        out_shape=jax.ShapeDtypeStruct((2, count, amps), jnp.float32),
        in_specs=[pl.BlockSpec(memory_space=pl.ANY)] * 4,
        out_specs=pl.BlockSpec(memory_space=pltpu.VMEM),
        scratch_shapes=[
            pltpu.VMEM((stages + 1, rows, 2 * width), jnp.bfloat16),
            pltpu.VMEM((stages, rows, 2 * width), jnp.bfloat16),
            pltpu.VMEM(gates.shape, jnp.bfloat16),
            pltpu.VMEM((stages, 4 * width, 2 * width), jnp.bfloat16),
            pltpu.VMEM((steps, 2, 2 * width, 2 * width), jnp.bfloat16),
            pltpu.VMEM((slots, 2, amps, rows), jnp.bfloat16),
            pltpu.VMEM((2, amps, width), jnp.float32),
            pltpu.VMEM((slots, 2, amps, width), jnp.bfloat16),
            pltpu.VMEM((slots, amps, 2 * width), jnp.float32),
            pltpu.VMEM((slots, 2, amps, 2 * width), jnp.float32),
            pltpu.VMEM((slots, 2, amps), jnp.float32),
            pltpu.VMEM((slots, 2, amps), jnp.float32),
            pltpu.VMEM((count, 2, amps), jnp.float32),
            pltpu.SemaphoreType.DMA((5,)),
            pltpu.SemaphoreType.DMA((stages, CHUNKS)),
            pltpu.SemaphoreType.DMA((stages, CHUNKS)),
            pltpu.SemaphoreType.DMA((slots, 3)),
            pltpu.SemaphoreType.DMA((slots, 3)),
            pltpu.SemaphoreType.DMA((slots,)),
            pltpu.SemaphoreType.DMA((slots,)),
            pltpu.SemaphoreType.DMA((count,)),
            pltpu.SemaphoreType.DMA((count,)),
        ],
        compiler_params=pltpu.CompilerParams(
            collective_id=0, has_side_effects=True, vmem_limit_bytes=60 * 2**20
        ),
    )(current, gates, closing_rows, closing_columns)
    return closed.reshape(2, count * amps)


def solution(mesh):
    placed = (
        P(None, "sx", "sy", None, None),
        P(),
        P(None, ("sx", "sy"), None),
        P(None, ("sx", "sy"), None),
    )
    return jax.shard_map(local, mesh=mesh, in_specs=placed, out_specs=P(), check_vma=False)
```

```python
import functools

import jax
import jax.numpy as jnp
from jax import lax
from jax.experimental import pallas as pl
from jax.experimental.pallas import tpu as pltpu
from jax.sharding import PartitionSpec as P

MESH = pl.DeviceIdType.MESH
CHUNKS = 8
LAG = 5
HOLD = 2
VECTOR = 5
FIRST = 6


def kernel(
    plan,
    x_hbm,
    g_hbm,
    u_hbm,
    v_hbm,
    out_ref,
    xs,
    xr,
    gates,
    mix,
    back,
    ubuf,
    vraw,
    vbuf,
    wbuf,
    acc,
    part,
    red,
    every,
    local_sem,
    xsend,
    xrecv,
    gsend,
    grecv,
    psend,
    precv,
    bsend,
    brecv,
):
    exchanges, gathers = plan
    rows, width2 = xs.shape[1:]
    width = width2 // 2
    slots, _, amps, _ = ubuf.shape
    step_rows = rows // CHUNKS
    coords = {"sx": lax.axis_index("sx"), "sy": lax.axis_index("sy")}

    def bit_of(axis, pos):
        return (coords[axis] // (1 << pos)) % 2

    def far(*flips):
        where = dict(coords)
        for axis, pos in flips:
            where[axis] = where[axis] + (1 << pos) * (1 - 2 * bit_of(axis, pos))
        return (where["sx"], where["sy"])

    copies = [
        pltpu.make_async_copy(x_hbm.at[0], xs.at[0, :, pl.ds(0, width)], local_sem.at[0]),
        pltpu.make_async_copy(x_hbm.at[1], xs.at[0, :, pl.ds(width, width)], local_sem.at[1]),
        pltpu.make_async_copy(v_hbm, vraw, local_sem.at[2]),
        pltpu.make_async_copy(u_hbm, ubuf.at[0], local_sem.at[3]),
        pltpu.make_async_copy(g_hbm, gates, local_sem.at[4]),
    ]
    for copy in copies:
        copy.start()

    barrier = pltpu.get_barrier_semaphore()
    peers = [(axis, pos) for axis, pos, _ in exchanges + gathers]
    for peer in peers:
        pl.semaphore_signal(barrier, inc=1, device_id=far(peer), device_id_type=MESH)
    copies[2].wait()
    vbuf[0] = vraw[...].astype(jnp.bfloat16)
    copies[0].wait()
    copies[1].wait()
    pl.semaphore_wait(barrier, len(peers))

    def x_copy(stage, chunk):
        here = pl.ds(chunk * step_rows, step_rows)
        return pltpu.make_async_remote_copy(
            src_ref=xs.at[stage, here],
            dst_ref=xr.at[stage, here],
            send_sem=xsend.at[stage, chunk],
            recv_sem=xrecv.at[stage, chunk],
            device_id=far(exchanges[stage][:2]),
            device_id_type=MESH,
        )

    def g_copy(step, slot, piece):
        landing = slot + (1 << step)
        if piece == 0:
            src, dst = vbuf.at[slot], vbuf.at[landing]
        else:
            src, dst = ubuf.at[slot, piece - 1], ubuf.at[landing, piece - 1]
        return pltpu.make_async_remote_copy(
            src_ref=src,
            dst_ref=dst,
            send_sem=gsend.at[landing, piece],
            recv_sem=grecv.at[landing, piece],
            device_id=far(gathers[step][:2]),
            device_id_type=MESH,
        )

    def offer(step):
        for piece in range(1, 3):
            g_copy(step, 0, piece).start()

    for chunk in range(CHUNKS):
        x_copy(0, chunk).start()
    for step in range(len(gathers)):
        g_copy(step, 0, 0).start()
    copies[3].wait()
    early = bit_of(*gathers[0][:2]) == bit_of(*exchanges[-1][:2])
    offer(0)
    for step in range(1, len(gathers)):
        offer(step)

    def arrive(slot, piece):
        step = slot.bit_length() - 1
        g_copy(step, slot - (1 << step), piece).wait_recv()
        for later in range(step + 1, len(gathers)):
            g_copy(later, slot, piece).start()

    copies[4].wait()
    for stage, (axis, pos, number) in enumerate(exchanges):
        sign = (1 - 2 * bit_of(axis, pos)).astype(jnp.float32).astype(jnp.bfloat16)
        for half in range(2):
            real, imag = gates[number, half, 0], gates[number, half, 1]
            if half:
                real, imag = real * sign, imag * sign
            base = half * width2
            mix[stage, pl.ds(base, width), pl.ds(0, width)] = real
            mix[stage, pl.ds(base, width), pl.ds(width, width)] = imag
            mix[stage, pl.ds(base + width, width), pl.ds(0, width)] = -imag
            mix[stage, pl.ds(base + width, width), pl.ds(width, width)] = real
    def build_back():
        for step, (axis, pos, number) in enumerate(gathers):
            sign = (2 * bit_of(axis, pos) - 1).astype(jnp.float32).astype(jnp.bfloat16)
            for half in range(2):
                real, imag = gates[number, half, 0], gates[number, half, 1]
                if half:
                    real, imag = real * sign, imag * sign
                back[step, half, pl.ds(0, width), pl.ds(0, width)] = real
                back[step, half, pl.ds(0, width), pl.ds(width, width)] = -imag
                back[step, half, pl.ds(width, width), pl.ds(0, width)] = imag
                back[step, half, pl.ds(width, width), pl.ds(width, width)] = real

    order = sorted(range(len(gathers)), key=lambda step: -gathers[step][2])

    def pull_back():
        values = [jnp.concatenate([vbuf[slot, 0], vbuf[slot, 1]], axis=-1) for slot in range(slots)]
        for place, step in enumerate(order):
            for half in range(2):
                chosen = [slot for slot in range(slots) if (slot >> step) & 1 == half]
                product = lax.dot_general(
                    jnp.concatenate([values[slot] for slot in chosen], axis=0),
                    back[step, half],
                    (((1,), (1,)), ((), ())),
                    preferred_element_type=jnp.float32,
                )
                for index, slot in enumerate(chosen):
                    rows_of = product[index * amps : (index + 1) * amps]
                    if place == len(order) - 1:
                        wbuf[slot] = rows_of
                    else:
                        values[slot] = rows_of.astype(jnp.bfloat16)

    def section(stage, chunk):
        x_copy(stage, chunk).wait_recv()
        here = pl.ds(chunk * step_rows, step_rows)
        joined = jnp.concatenate([xs[stage, here], xr[stage, here]], axis=-1)
        xs[stage + 1, here] = jnp.dot(
            joined, mix[stage], preferred_element_type=jnp.float32
        ).astype(jnp.bfloat16)
        if stage + 1 < len(exchanges):
            x_copy(stage + 1, chunk).start()

    def spread(events, moments):
        size = len(moments)
        return {
            moment: events[len(events) * place // size : len(events) * (place + 1) // size]
            for place, moment in enumerate(moments)
        }

    total = CHUNKS + LAG * (len(exchanges) - 1)
    wait_tick = total - CHUNKS + FIRST - 1
    half = slots // 2
    vectors = [(slot, 0) for slot in range(1, slots)]
    relays = [(slot, piece) for piece in range(1, 3) for slot in range(2, half) if slot % 2 == 0]
    late = [(slot, piece) for piece in range(1, 3) for slot in range(1, half) if slot % 2]
    late.sort(key=lambda event: (event[1] + event[0].bit_count(), event[0]))
    ends = [(slot, piece) for piece in range(1, 3) for slot in range(half, slots)]
    at_tick = spread(vectors, range(VECTOR))
    for events in (spread(relays, range(1, HOLD + 1)), spread(late, range(HOLD + 1, wait_tick + 1))):
        for moment in events:
            at_tick[moment] = at_tick.get(moment, []) + events[moment]

    def gather_rows(start, stop):
        return jnp.dot(
            ubuf[:, :, :, start:stop].reshape(slots * 2 * amps, stop - start),
            xs[len(exchanges), start:stop],
            preferred_element_type=jnp.float32,
        ).reshape(slots, 2, amps, 2 * width)

    for tick in range(total):
        for stage in range(len(exchanges)):
            chunk = tick - LAG * stage
            if 0 <= chunk < CHUNKS:
                section(stage, chunk)
        if tick == HOLD:
            pass
        for event in at_tick.get(tick, ()):
            arrive(*event)
        if tick == VECTOR - 1:
            build_back()
        if tick == VECTOR:
            pull_back()
        if tick == wait_tick:
            for event in ends:
                arrive(*event)
            acc[...] = gather_rows(0, FIRST * step_rows)

    def p_copy(slot):
        flips = [gathers[step][:2] for step in range(len(gathers)) if (slot >> step) & 1]
        return pltpu.make_async_remote_copy(
            src_ref=part.at[slot],
            dst_ref=red.at[slot],
            send_sem=psend.at[slot],
            recv_sem=precv.at[slot],
            device_id=far(*flips),
            device_id_type=MESH,
        )

    def fold(values):
        lanes = 128
        total_ = values[:, :lanes]
        for start in range(lanes, width, lanes):
            total_ = total_ + values[:, start : start + lanes]
        return jnp.sum(total_.T, axis=0, keepdims=True)

    acc[...] += gather_rows(FIRST * step_rows, rows)
    for slot in reversed(range(slots)):
        by_real, by_imag = acc[slot, 0], acc[slot, 1]
        proj_real = by_real[:, :width] - by_imag[:, width:]
        proj_imag = by_real[:, width:] + by_imag[:, :width]
        w_real, w_imag = wbuf[slot, :, :width], wbuf[slot, :, width:]
        part[slot, 0:1] = fold(proj_real * w_real - proj_imag * w_imag)
        part[slot, 1:2] = fold(proj_real * w_imag + proj_imag * w_real)
        if slot:
            p_copy(slot).start()

    result = part[0]
    for slot in range(1, slots):
        p_copy(slot).wait_recv()
    for slot in range(1, slots):
        result = result + red[slot]
    count_y = lax.axis_size("sy")
    count = lax.axis_size("sx") * count_y
    rank = coords["sx"] * count_y + coords["sy"]
    every[pl.ds(rank, 1)] = result[None]

    def b_copy(offset):
        other = (rank + offset) % count
        return pltpu.make_async_remote_copy(
            src_ref=every.at[rank],
            dst_ref=every.at[rank],
            send_sem=bsend.at[offset],
            recv_sem=brecv.at[offset],
            device_id=(other // count_y, other % count_y),
            device_id_type=MESH,
        )

    @pl.loop(1, count)
    def _(offset):
        b_copy(offset).start()


    for stage in range(len(exchanges)):
        for chunk in range(CHUNKS):
            x_copy(stage, chunk).wait_send()
    for step in range(len(gathers)):
        for slot in range(1 << step):
            for piece in range(3):
                g_copy(step, slot, piece).wait_send()
    for slot in range(1, slots):
        p_copy(slot).wait_send()

    @pl.loop(1, count)
    def _(offset):
        b_copy(offset).wait()

    out_ref[0] = every[:, 0, :]
    out_ref[1] = every[:, 1, :]


def local(tensors, gates, closing_rows, closing_columns):
    current = tensors[:, 0, 0]
    rows, width = current.shape[1:]
    amps = closing_rows.shape[1]
    bits_x = lax.axis_size("sx").bit_length() - 1
    bits_y = lax.axis_size("sy").bit_length() - 1
    exchanges = [("sx", pos, pos) for pos in range(bits_x - 1)]
    gathers = [("sx", bits_x - 1, bits_x - 1)]
    gathers += [("sy", pos, bits_x + pos) for pos in reversed(range(bits_y))]
    stages, steps = len(exchanges), len(gathers)
    slots = 1 << steps
    count = lax.axis_size("sx") * lax.axis_size("sy")
    closed = pl.pallas_call(
        functools.partial(kernel, (exchanges, gathers)),
        out_shape=jax.ShapeDtypeStruct((2, count, amps), jnp.float32),
        in_specs=[pl.BlockSpec(memory_space=pl.ANY)] * 4,
        out_specs=pl.BlockSpec(memory_space=pltpu.VMEM),
        scratch_shapes=[
            pltpu.VMEM((stages + 1, rows, 2 * width), jnp.bfloat16),
            pltpu.VMEM((stages, rows, 2 * width), jnp.bfloat16),
            pltpu.VMEM(gates.shape, jnp.bfloat16),
            pltpu.VMEM((stages, 4 * width, 2 * width), jnp.bfloat16),
            pltpu.VMEM((steps, 2, 2 * width, 2 * width), jnp.bfloat16),
            pltpu.VMEM((slots, 2, amps, rows), jnp.bfloat16),
            pltpu.VMEM((2, amps, width), jnp.float32),
            pltpu.VMEM((slots, 2, amps, width), jnp.bfloat16),
            pltpu.VMEM((slots, amps, 2 * width), jnp.float32),
            pltpu.VMEM((slots, 2, amps, 2 * width), jnp.float32),
            pltpu.VMEM((slots, 2, amps), jnp.float32),
            pltpu.VMEM((slots, 2, amps), jnp.float32),
            pltpu.VMEM((count, 2, amps), jnp.float32),
            pltpu.SemaphoreType.DMA((5,)),
            pltpu.SemaphoreType.DMA((stages, CHUNKS)),
            pltpu.SemaphoreType.DMA((stages, CHUNKS)),
            pltpu.SemaphoreType.DMA((slots, 3)),
            pltpu.SemaphoreType.DMA((slots, 3)),
            pltpu.SemaphoreType.DMA((slots,)),
            pltpu.SemaphoreType.DMA((slots,)),
            pltpu.SemaphoreType.DMA((count,)),
            pltpu.SemaphoreType.DMA((count,)),
        ],
        compiler_params=pltpu.CompilerParams(
            collective_id=0, has_side_effects=True, vmem_limit_bytes=60 * 2**20
        ),
    )(current, gates, closing_rows, closing_columns)
    return closed.reshape(2, count * amps)


def solution(mesh):
    placed = (
        P(None, "sx", "sy", None, None),
        P(),
        P(None, ("sx", "sy"), None),
        P(None, ("sx", "sy"), None),
    )
    return jax.shard_map(local, mesh=mesh, in_specs=placed, out_specs=P(), check_vma=False)
```

```python
import functools

import jax
import jax.numpy as jnp
from jax import lax
from jax.experimental import pallas as pl
from jax.experimental.pallas import tpu as pltpu
from jax.sharding import PartitionSpec as P

MESH = pl.DeviceIdType.MESH
CHUNKS = 8
LAG = 5
HOLD = 2
VECTOR = 5
PARTS = 4
FIRST = 6


def kernel(
    plan,
    x_hbm,
    g_hbm,
    u_hbm,
    v_hbm,
    out_ref,
    xs,
    xr,
    gates,
    mix,
    back,
    ubuf,
    vraw,
    vbuf,
    wbuf,
    acc,
    part,
    red,
    every,
    local_sem,
    xsend,
    xrecv,
    gsend,
    grecv,
    psend,
    precv,
    bsend,
    brecv,
):
    exchanges, gathers = plan
    rows, width2 = xs.shape[1:]
    width = width2 // 2
    slots, _, amps, _ = ubuf.shape
    step_rows = rows // CHUNKS
    coords = {"sx": lax.axis_index("sx"), "sy": lax.axis_index("sy")}

    def bit_of(axis, pos):
        return (coords[axis] // (1 << pos)) % 2

    def far(*flips):
        where = dict(coords)
        for axis, pos in flips:
            where[axis] = where[axis] + (1 << pos) * (1 - 2 * bit_of(axis, pos))
        return (where["sx"], where["sy"])

    copies = [
        pltpu.make_async_copy(x_hbm.at[0], xs.at[0, :, pl.ds(0, width)], local_sem.at[0]),
        pltpu.make_async_copy(x_hbm.at[1], xs.at[0, :, pl.ds(width, width)], local_sem.at[1]),
        pltpu.make_async_copy(v_hbm, vraw, local_sem.at[2]),
        pltpu.make_async_copy(u_hbm, ubuf.at[0], local_sem.at[3]),
        pltpu.make_async_copy(g_hbm, gates, local_sem.at[4]),
    ]
    for copy in copies:
        copy.start()

    barrier = pltpu.get_barrier_semaphore()
    peers = [(axis, pos) for axis, pos, _ in exchanges + gathers]
    for peer in peers:
        pl.semaphore_signal(barrier, inc=1, device_id=far(peer), device_id_type=MESH)
    copies[2].wait()
    vbuf[0] = vraw[...].astype(jnp.bfloat16)
    copies[0].wait()
    copies[1].wait()
    pl.semaphore_wait(barrier, len(peers))

    def x_copy(stage, chunk):
        here = pl.ds(chunk * step_rows, step_rows)
        return pltpu.make_async_remote_copy(
            src_ref=xs.at[stage, here],
            dst_ref=xr.at[stage, here],
            send_sem=xsend.at[stage, chunk],
            recv_sem=xrecv.at[stage, chunk],
            device_id=far(exchanges[stage][:2]),
            device_id_type=MESH,
        )

    def g_copy(step, slot, piece):
        landing = slot + (1 << step)
        if piece == 0:
            src, dst = vbuf.at[slot], vbuf.at[landing]
        else:
            span = pl.ds((piece - 1) * (rows // PARTS), rows // PARTS)
            src, dst = ubuf.at[slot, :, :, span], ubuf.at[landing, :, :, span]
        return pltpu.make_async_remote_copy(
            src_ref=src,
            dst_ref=dst,
            send_sem=gsend.at[landing, piece],
            recv_sem=grecv.at[landing, piece],
            device_id=far(gathers[step][:2]),
            device_id_type=MESH,
        )

    def offer(step):
        for piece in range(1, PARTS + 1):
            g_copy(step, 0, piece).start()

    for chunk in range(CHUNKS):
        x_copy(0, chunk).start()
    for step in range(len(gathers)):
        g_copy(step, 0, 0).start()
    copies[3].wait()
    early = bit_of(*gathers[0][:2]) == bit_of(*exchanges[-1][:2])
    offer(0)
    for step in range(1, len(gathers)):
        offer(step)

    def arrive(slot, piece):
        step = slot.bit_length() - 1
        g_copy(step, slot - (1 << step), piece).wait_recv()
        for later in range(step + 1, len(gathers)):
            g_copy(later, slot, piece).start()

    copies[4].wait()
    for stage, (axis, pos, number) in enumerate(exchanges):
        sign = (1 - 2 * bit_of(axis, pos)).astype(jnp.float32).astype(jnp.bfloat16)
        for half in range(2):
            real, imag = gates[number, half, 0], gates[number, half, 1]
            if half:
                real, imag = real * sign, imag * sign
            base = half * width2
            mix[stage, pl.ds(base, width), pl.ds(0, width)] = real
            mix[stage, pl.ds(base, width), pl.ds(width, width)] = imag
            mix[stage, pl.ds(base + width, width), pl.ds(0, width)] = -imag
            mix[stage, pl.ds(base + width, width), pl.ds(width, width)] = real
    def build_back():
        for step, (axis, pos, number) in enumerate(gathers):
            sign = (2 * bit_of(axis, pos) - 1).astype(jnp.float32).astype(jnp.bfloat16)
            for half in range(2):
                real, imag = gates[number, half, 0], gates[number, half, 1]
                if half:
                    real, imag = real * sign, imag * sign
                back[step, half, pl.ds(0, width), pl.ds(0, width)] = real
                back[step, half, pl.ds(0, width), pl.ds(width, width)] = -imag
                back[step, half, pl.ds(width, width), pl.ds(0, width)] = imag
                back[step, half, pl.ds(width, width), pl.ds(width, width)] = real

    order = sorted(range(len(gathers)), key=lambda step: -gathers[step][2])

    def pull_back():
        values = [jnp.concatenate([vbuf[slot, 0], vbuf[slot, 1]], axis=-1) for slot in range(slots)]
        for place, step in enumerate(order):
            for half in range(2):
                chosen = [slot for slot in range(slots) if (slot >> step) & 1 == half]
                product = lax.dot_general(
                    jnp.concatenate([values[slot] for slot in chosen], axis=0),
                    back[step, half],
                    (((1,), (1,)), ((), ())),
                    preferred_element_type=jnp.float32,
                )
                for index, slot in enumerate(chosen):
                    rows_of = product[index * amps : (index + 1) * amps]
                    if place == len(order) - 1:
                        wbuf[slot] = rows_of
                    else:
                        values[slot] = rows_of.astype(jnp.bfloat16)

    def section(stage, chunk):
        x_copy(stage, chunk).wait_recv()
        here = pl.ds(chunk * step_rows, step_rows)
        joined = jnp.concatenate([xs[stage, here], xr[stage, here]], axis=-1)
        xs[stage + 1, here] = jnp.dot(
            joined, mix[stage], preferred_element_type=jnp.float32
        ).astype(jnp.bfloat16)
        if stage + 1 < len(exchanges):
            x_copy(stage + 1, chunk).start()

    def spread(events, moments):
        size = len(moments)
        return {
            moment: events[len(events) * place // size : len(events) * (place + 1) // size]
            for place, moment in enumerate(moments)
        }

    total = CHUNKS + LAG * (len(exchanges) - 1)
    wait_tick = total - CHUNKS + FIRST - 1
    half = slots // 2
    vectors = [(slot, 0) for slot in range(1, slots)]
    relays = [(slot, piece) for piece in range(1, PARTS + 1) for slot in range(2, half) if slot % 2 == 0]
    late = [(slot, piece) for piece in range(1, PARTS + 1) for slot in range(1, half) if slot % 2]
    late.sort(key=lambda event: (event[1] + event[0].bit_count(), event[0]))
    tail = [event for event in late if event[1] == PARTS and event[0].bit_count() > 1]
    late = [event for event in late if event not in tail]
    ends = [(slot, piece) for piece in range(1, PARTS + 1) for slot in range(half, slots)]
    at_tick = spread(vectors, range(VECTOR))
    for events in (spread(relays, range(1, HOLD + 1)), spread(late, range(HOLD + 1, wait_tick + 1))):
        for moment in events:
            at_tick[moment] = at_tick.get(moment, []) + events[moment]

    def gather_rows(start, stop):
        return jnp.dot(
            ubuf[:, :, :, start:stop].reshape(slots * 2 * amps, stop - start),
            xs[len(exchanges), start:stop],
            preferred_element_type=jnp.float32,
        ).reshape(slots, 2, amps, 2 * width)

    for tick in range(total):
        for stage in range(len(exchanges)):
            chunk = tick - LAG * stage
            if 0 <= chunk < CHUNKS:
                section(stage, chunk)
        if tick == HOLD:
            pass
        for event in at_tick.get(tick, ()):
            arrive(*event)
        if tick == VECTOR - 1:
            build_back()
        if tick == VECTOR:
            pull_back()
        if tick == wait_tick:
            for event in ends:
                if event[1] < PARTS:
                    arrive(*event)
            acc[...] = gather_rows(0, FIRST * step_rows)
            for event in tail + ends:
                if event[1] == PARTS:
                    arrive(*event)

    def p_copy(slot):
        flips = [gathers[step][:2] for step in range(len(gathers)) if (slot >> step) & 1]
        return pltpu.make_async_remote_copy(
            src_ref=part.at[slot],
            dst_ref=red.at[slot],
            send_sem=psend.at[slot],
            recv_sem=precv.at[slot],
            device_id=far(*flips),
            device_id_type=MESH,
        )

    def fold(values):
        lanes = 128
        total_ = values[:, :lanes]
        for start in range(lanes, width, lanes):
            total_ = total_ + values[:, start : start + lanes]
        return jnp.sum(total_.T, axis=0, keepdims=True)

    acc[...] += gather_rows(FIRST * step_rows, rows)
    for slot in reversed(range(slots)):
        by_real, by_imag = acc[slot, 0], acc[slot, 1]
        proj_real = by_real[:, :width] - by_imag[:, width:]
        proj_imag = by_real[:, width:] + by_imag[:, :width]
        w_real, w_imag = wbuf[slot, :, :width], wbuf[slot, :, width:]
        part[slot, 0:1] = fold(proj_real * w_real - proj_imag * w_imag)
        part[slot, 1:2] = fold(proj_real * w_imag + proj_imag * w_real)
        if slot:
            p_copy(slot).start()

    result = part[0]
    for slot in range(1, slots):
        p_copy(slot).wait_recv()
    for slot in range(1, slots):
        result = result + red[slot]
    count_y = lax.axis_size("sy")
    count = lax.axis_size("sx") * count_y
    rank = coords["sx"] * count_y + coords["sy"]
    every[pl.ds(rank, 1)] = result[None]

    def b_copy(offset):
        other = (rank + offset) % count
        return pltpu.make_async_remote_copy(
            src_ref=every.at[rank],
            dst_ref=every.at[rank],
            send_sem=bsend.at[offset],
            recv_sem=brecv.at[offset],
            device_id=(other // count_y, other % count_y),
            device_id_type=MESH,
        )

    @pl.loop(1, count)
    def _(offset):
        b_copy(offset).start()


    for stage in range(len(exchanges)):
        for chunk in range(CHUNKS):
            x_copy(stage, chunk).wait_send()
    for step in range(len(gathers)):
        for slot in range(1 << step):
            for piece in range(PARTS + 1):
                g_copy(step, slot, piece).wait_send()
    for slot in range(1, slots):
        p_copy(slot).wait_send()

    @pl.loop(1, count)
    def _(offset):
        b_copy(offset).wait()

    out_ref[0] = every[:, 0, :]
    out_ref[1] = every[:, 1, :]


def local(tensors, gates, closing_rows, closing_columns):
    current = tensors[:, 0, 0]
    rows, width = current.shape[1:]
    amps = closing_rows.shape[1]
    bits_x = lax.axis_size("sx").bit_length() - 1
    bits_y = lax.axis_size("sy").bit_length() - 1
    exchanges = [("sx", pos, pos) for pos in range(bits_x - 1)]
    gathers = [("sx", bits_x - 1, bits_x - 1)]
    gathers += [("sy", pos, bits_x + pos) for pos in reversed(range(bits_y))]
    stages, steps = len(exchanges), len(gathers)
    slots = 1 << steps
    count = lax.axis_size("sx") * lax.axis_size("sy")
    closed = pl.pallas_call(
        functools.partial(kernel, (exchanges, gathers)),
        out_shape=jax.ShapeDtypeStruct((2, count, amps), jnp.float32),
        in_specs=[pl.BlockSpec(memory_space=pl.ANY)] * 4,
        out_specs=pl.BlockSpec(memory_space=pltpu.VMEM),
        scratch_shapes=[
            pltpu.VMEM((stages + 1, rows, 2 * width), jnp.bfloat16),
            pltpu.VMEM((stages, rows, 2 * width), jnp.bfloat16),
            pltpu.VMEM(gates.shape, jnp.bfloat16),
            pltpu.VMEM((stages, 4 * width, 2 * width), jnp.bfloat16),
            pltpu.VMEM((steps, 2, 2 * width, 2 * width), jnp.bfloat16),
            pltpu.VMEM((slots, 2, amps, rows), jnp.bfloat16),
            pltpu.VMEM((2, amps, width), jnp.float32),
            pltpu.VMEM((slots, 2, amps, width), jnp.bfloat16),
            pltpu.VMEM((slots, amps, 2 * width), jnp.float32),
            pltpu.VMEM((slots, 2, amps, 2 * width), jnp.float32),
            pltpu.VMEM((slots, 2, amps), jnp.float32),
            pltpu.VMEM((slots, 2, amps), jnp.float32),
            pltpu.VMEM((count, 2, amps), jnp.float32),
            pltpu.SemaphoreType.DMA((5,)),
            pltpu.SemaphoreType.DMA((stages, CHUNKS)),
            pltpu.SemaphoreType.DMA((stages, CHUNKS)),
            pltpu.SemaphoreType.DMA((slots, PARTS + 1)),
            pltpu.SemaphoreType.DMA((slots, PARTS + 1)),
            pltpu.SemaphoreType.DMA((slots,)),
            pltpu.SemaphoreType.DMA((slots,)),
            pltpu.SemaphoreType.DMA((count,)),
            pltpu.SemaphoreType.DMA((count,)),
        ],
        compiler_params=pltpu.CompilerParams(
            collective_id=0, has_side_effects=True, vmem_limit_bytes=60 * 2**20
        ),
    )(current, gates, closing_rows, closing_columns)
    return closed.reshape(2, count * amps)


def solution(mesh):
    placed = (
        P(None, "sx", "sy", None, None),
        P(),
        P(None, ("sx", "sy"), None),
        P(None, ("sx", "sy"), None),
    )
    return jax.shard_map(local, mesh=mesh, in_specs=placed, out_specs=P(), check_vma=False)
```
